256 devices in a mesh: section: 16 (over z, core), expert: 16 (over x, y).
Axes of the slice: x: 4, y: 4, z: 8, core: 2. Of those that a mesh axis runs over, the one named last changes fastest.
Arguments:
- state: bfloat16 [16, 2048, 2048], P('section', 'expert'), may hold values from -6 to 6
- norm_gain: float32 [16, 2048], P('section'), may hold values from 0.25 to 1.75
- expert_in: bfloat16 [16, 16, 2048, 1536], P('section', 'expert'), may hold values from -0.125 to 0.125
- expert_out: bfloat16 [16, 16, 768, 2048], P('section', 'expert'), may hold values from -0.21875 to 0.21875
- route_ids: int32 [3, 16, 2048, 6], P(None, 'section', 'expert'), may hold values from 0 to 63, all different within a row
- route_weights: float32 [3, 16, 2048, 6], P(None, 'section', 'expert'), may hold values from 0.3 to 3
Outputs:
- state_out: bfloat16 [16, 2048, 2048], P('section', 'expert')
The draws below stay inside these ranges and needn't reach their ends.
Inputs may be any that keep to these rules, and one draw needn't show every extreme that they name: `route_ids`: each token names 6 different experts.
All inputs are finite; a program needn't handle non-finite values.
Results may differ from the reference program's by a relative error of at most 0.02.
Values may be sent and summed in bfloat16 or wider, within the bound.
A program may use at most 64 MiB of HBM per device.

```python
import math
from functools import partial
import jax
import jax.numpy as jnp
from jax import lax

D = 2048
ROUTED = 64
TOP = 6
FF = 768
TICKS = 3
TOK_DEV = 128
CAP = 32
EXPERTS = 16
TOKENS = 2048
N_SECTION = 16
N_EXPERT = 16


def steps_of(stream_key, extent, pieces, least, high):
    gain, own = 1.0, jax.random.fold_in(stream_key, 6)
    for position, parts in pieces:
        draws = jnp.exp(jax.random.uniform(jax.random.fold_in(own, position), (parts,), jnp.float32, least / len(pieces), high / len(pieces)))
        gain = gain * jnp.repeat(draws, extent[position] // parts).reshape([-1 if axis == position else 1 for axis in range(len(extent))])
    return gain


def choose_distinct(rng, rows, count, top, lift):
    ranking = jax.random.permutation(jax.random.fold_in(rng, 1), count)
    boost = ranking
    for power in range(3):
        boost = boost * boost // count
    boost = boost * lift // count
    lots = jax.random.randint(jax.random.fold_in(rng, 2), (rows, count), 0, 4096) + boost
    fixed_rows = jax.random.permutation(jax.random.fold_in(rng, 3), rows)[jnp.arange(count) % rows]
    lots = jnp.where(jnp.arange(rows)[:, None] == fixed_rows[None, :], 1 << 14, lots)
    priority = lots * count + jnp.arange(count)
    return lax.top_k(priority.astype(jnp.int32), top)[1].astype(jnp.int32)


def noise(stream_key, extent, deviation, most, pieces=(), kind=jnp.bfloat16):
    gain = steps_of(stream_key, extent, pieces, -0.22, 0.18) if pieces else 1.0
    result = jax.random.normal(stream_key, extent, jnp.float32) * deviation * gain
    return jnp.minimum(jnp.maximum(result, -most), most).astype(kind)


def setup_inputs(seed: int = 0) -> dict:
    splits = jax.random.split(jax.random.key(seed), 7)
    state = noise(splits[0], (N_SECTION, TOKENS, D), 1.0, 6.0, ((0, 16), (1, 16)))
    norm_gain = jnp.clip(1.0 + 0.15 * jax.random.normal(splits[1], (N_SECTION, D), jnp.float32), 0.25, 1.75)
    expert_in = noise(splits[2], (N_SECTION, EXPERTS, D, 2 * FF), D ** -0.5, 0.125, ((0, 16), (1, 16)))
    expert_out = noise(splits[3], (N_SECTION, EXPERTS, FF, D), FF ** -0.5, 0.21875, ((0, 16), (1, 16)))
    route_ids = choose_distinct(splits[4], TICKS * N_SECTION * TOKENS, ROUTED, TOP, 1536).reshape((TICKS, N_SECTION, TOKENS, TOP))
    route_weights = jnp.clip(jnp.exp(math.log(3.0) - 2.3025851 * jax.random.uniform(splits[5], (TICKS, N_SECTION, TOKENS, TOP), jnp.float32) ** steps_of(splits[5], (TICKS, N_SECTION, TOKENS, TOP), ((1, 16), (2, 16)), -0.2, 0.2)), 0.3, 3.0)
    return dict(state=state, norm_gain=norm_gain, expert_in=expert_in, expert_out=expert_out, route_ids=route_ids, route_weights=route_weights)


epsilon = 1e-06

def normalize(hidden, gain_row):
    widened = hidden.astype(jnp.float32)
    rescale = lax.rsqrt(lax.optimization_barrier(jnp.mean(widened * widened, axis=-1, keepdims=True)) + epsilon)
    return (widened * rescale * gain_row).astype(jnp.bfloat16)

def slot_tables(chosen, experts, capacity):
    window = jnp.arange(experts, dtype=jnp.int32)
    choice_hits = (chosen[:, :, None] == window[None, None, :]).astype(jnp.int32)
    picked = lax.optimization_barrier(jnp.sum(choice_hits, axis=1))
    rank_table = jnp.cumsum(picked, axis=0) - picked
    kept_table = picked * (rank_table < capacity).astype(jnp.int32)
    slot_index = jnp.arange(capacity, dtype=jnp.int32)
    slot_match = kept_table[:, :, None] * (rank_table[:, :, None] == slot_index[None, None, :]).astype(jnp.int32)
    positions = jnp.arange(chosen.shape[0], dtype=jnp.int32)
    token_at = lax.optimization_barrier(jnp.sum(slot_match * positions[:, None, None], axis=0))
    filled = lax.optimization_barrier(jnp.sum(slot_match, axis=0))
    kept_hits = choice_hits * kept_table[:, None, :]
    kept_choice = lax.optimization_barrier(jnp.sum(kept_hits, axis=2))
    flat_slot = lax.optimization_barrier(jnp.sum(kept_hits * (window[None, None, :] * capacity + rank_table[:, None, :]), axis=2))
    return (token_at, filled, flat_slot, kept_choice)

def expert_forward(token_rows, inner_weight, outer_weight):
    projected = jnp.dot(token_rows, inner_weight, preferred_element_type=jnp.float32)
    hidden_units = outer_weight.shape[0]
    activated = (jax.nn.silu(projected[:, :hidden_units]) * projected[:, hidden_units:]).astype(jnp.bfloat16)
    return jnp.dot(activated, outer_weight, preferred_element_type=jnp.float32).astype(jnp.bfloat16)

def serve_expert(operands):
    arrived, inner_one, outer_one = operands
    token_rows = arrived.reshape(-1, arrived.shape[-1])
    return expert_forward(token_rows, inner_one, outer_one).reshape(arrived.shape)

def layer(operands):
    hidden, gain_row, inner_weight, outer_weight, chosen, weights = operands
    normed = normalize(hidden, gain_row).reshape(N_EXPERT, TOK_DEV, D)
    tables = jax.vmap(partial(slot_tables, experts=EXPERTS, capacity=CAP))
    token_at, filled, flat_slot, kept_choice = tables(chosen.reshape(N_EXPERT, TOK_DEV, TOP))
    taker = jax.vmap(partial(jnp.take, axis=0))
    outbound = taker(normed, token_at) * filled[:, :, :, None].astype(jnp.bfloat16)
    served = lax.map(serve_expert, (jnp.swapaxes(outbound, 0, 1), inner_weight, outer_weight))
    returned = jnp.swapaxes(served, 0, 1).reshape(N_EXPERT, EXPERTS * CAP, D)
    picked_rows = taker(returned, flat_slot)
    mixing = weights.reshape(N_EXPERT, TOK_DEV, TOP) * kept_choice.astype(weights.dtype)
    branch = jnp.einsum('btk,btkd->btd', mixing, picked_rows.astype(jnp.float32))
    return (hidden.astype(jnp.float32) + branch.reshape(TOKENS, D)).astype(jnp.bfloat16)

def reference(state, norm_gain, expert_in, expert_out, route_ids, route_weights):
    holding = state
    for tick_index in range(TICKS):
        moved = lax.map(layer, (holding, norm_gain, expert_in, expert_out, route_ids[tick_index], route_weights[tick_index]))
        holding = jnp.roll(moved, 1, axis=0)
    return holding
```

```python
import functools

import jax
import jax.numpy as jnp
from jax import lax
from jax.experimental import pallas as pl
from jax.experimental.pallas import tpu as pltpu
from jax.sharding import PartitionSpec as P

MESH = pl.DeviceIdType.MESH
BF16 = jnp.bfloat16
F32 = jnp.float32

EPSILON = 1e-06
SIDE = 4
SLOTS = 32
GROUP = 4
CHUNKS = 4
ORDER = (
    (0, 0), (0, 1), (0, 3), (1, 0), (3, 0), (0, 2), (1, 1), (1, 3),
    (2, 0), (3, 1), (3, 3), (1, 2), (2, 1), (2, 3), (3, 2), (2, 2),
)


def body(
    ids_ref, weights_ref, gain_ref, state_ref, inner_hbm, outer_hbm, out_ref,
    hid, normed, sbuf, rbuf, obuf, ret, acc, ybuf, inner, outer, act, rank_ref, mix_ref, pick, mixing,
    load_sem, weight_sem, out_sem, dispatch_send, dispatch_recv, ret_send, ret_recv, y_send, y_recv,
):
    ticks, tokens = ids_ref.shape[0], ids_ref.shape[2]
    width = gain_ref.shape[1]
    part = width // CHUNKS
    ff = outer.shape[0]
    peers = SIDE * SIDE
    groups = peers // GROUP
    section = lax.axis_index("section")
    sections = lax.axis_size("section")
    me = lax.axis_index("expert")
    my_x, my_y = me // SIDE, lax.rem(me, SIDE)

    def at_offset(dx, dy):
        return lax.rem(my_x + dx + SIDE, SIDE) * SIDE + lax.rem(my_y + dy + SIDE, SIDE)

    target = [at_offset(dx, dy) for dx, dy in ORDER]
    source = [at_offset(-dx, -dy) for dx, dy in ORDER]
    following = lax.rem(section + 1, sections)
    previous = lax.rem(section + sections - 1, sections)

    barrier = pltpu.get_barrier_semaphore()
    for k in range(1, peers):
        pl.semaphore_signal(barrier, 1, device_id={"expert": target[k]}, device_id_type=MESH)
    pl.semaphore_signal(barrier, 1, device_id={"section": following}, device_id_type=MESH)
    pl.semaphore_signal(barrier, 1, device_id={"section": previous}, device_id_type=MESH)

    loads = [
        pltpu.make_async_copy(state_ref.at[:, pl.ds(c * part, part)], hid.at[0, c], load_sem.at[c])
        for c in range(CHUNKS)
    ]
    for load in loads:
        load.start()
    inner_load = pltpu.make_async_copy(inner_hbm, inner, weight_sem.at[0])
    outer_load = pltpu.make_async_copy(outer_hbm, outer, weight_sem.at[1])
    inner_load.start()
    outer_load.start()

    expert_of = lax.broadcasted_iota(jnp.int32, (peers, tokens), 0)
    earlier = (
        lax.broadcasted_iota(jnp.int32, (tokens, tokens), 0)
        < lax.broadcasted_iota(jnp.int32, (tokens, tokens), 1)
    ).astype(F32).astype(BF16)
    slot_of = lax.broadcasted_iota(jnp.int32, (SLOTS, tokens), 0).astype(F32)

    def tables(t, carry):
        ids, weights = ids_ref[t], weights_ref[t]
        picked = jnp.zeros((peers, tokens), F32)
        mix = jnp.zeros((peers, tokens), F32)
        for k in range(ids.shape[0]):
            hit = ids[k : k + 1] == expert_of
            picked = jnp.where(hit, 1.0, picked)
            mix = jnp.where(hit, weights[k : k + 1], mix)
        rank = jnp.dot(picked.astype(BF16), earlier, preferred_element_type=F32)
        rank_ref[...] = jnp.where(picked > 0.0, rank, -1.0)
        mix_ref[...] = mix
        for g in range(groups):
            rows = []
            for j in range(GROUP):
                k = g * GROUP + j
                match = rank_ref[pl.ds(target[k], 1), :] == slot_of
                pick[t, k] = jnp.where(match, 1.0, 0.0).astype(BF16)
                rows.append(jnp.where(match, mix_ref[pl.ds(target[k], 1), :], 0.0))
            mixing[t, g] = jnp.concatenate(rows, axis=0).T.astype(BF16)
        return carry

    lax.fori_loop(0, ticks, tables, 0)
    for load in loads:
        load.wait()
    pl.semaphore_wait(barrier, peers + 1)

    def tick(t, carry):
        squares = jnp.zeros((tokens, 1), F32)
        for c in range(CHUNKS):
            h = hid[t, c].astype(F32)
            squares = squares + jnp.sum(h * h, axis=-1, keepdims=True)
        rescale = lax.rsqrt(squares / width + EPSILON)
        for c in range(CHUNKS):
            columns = slice(c * part, (c + 1) * part)
            normed[:, columns] = (hid[t, c].astype(F32) * rescale * gain_ref[:, columns]).astype(BF16)

        sends = []
        for g in range(groups):
            choose = pick[t, g * GROUP : (g + 1) * GROUP].reshape(GROUP * SLOTS, tokens)
            for c in range(CHUNKS):
                columns = slice(c * part, (c + 1) * part)
                rows = jnp.dot(choose, normed[:, columns], preferred_element_type=F32).astype(BF16)
                for j in range(GROUP):
                    k = g * GROUP + j
                    piece = rows[j * SLOTS : (j + 1) * SLOTS]
                    if k == 0:
                        rbuf[t, 0, :, columns] = piece
                    else:
                        sbuf[k, :, columns] = piece
            for k in range(max(g * GROUP, 1), (g + 1) * GROUP):
                send = pltpu.make_async_remote_copy(
                    sbuf.at[k], rbuf.at[t, k], dispatch_send.at[k], dispatch_recv.at[t, k],
                    device_id={"expert": target[k]}, device_id_type=MESH,
                )
                send.start()
                sends.append(send)

        @pl.when(t == 0)
        def _():
            inner_load.wait()
            outer_load.wait()

        returns = []
        for g in range(groups):
            first = g * GROUP
            for k in range(max(first, 1), first + GROUP):
                sends[k - 1].wait_recv()
            for n in range(ff // 256):
                gate_columns = slice(n * 256, (n + 1) * 256)
                up_columns = slice(ff + n * 256, ff + (n + 1) * 256)
                rows = rbuf[t, first : first + GROUP].reshape(GROUP * SLOTS, width)
                gate = jnp.dot(rows, inner[:, gate_columns], preferred_element_type=F32)
                up = jnp.dot(rows, inner[:, up_columns], preferred_element_type=F32)
                act[:, gate_columns] = (gate / (1.0 + jnp.exp(-gate)) * up).astype(BF16)
            for c in range(CHUNKS):
                served = jnp.dot(
                    act[...], outer[:, c * part : (c + 1) * part], preferred_element_type=F32
                ).astype(BF16)
                for j in range(GROUP):
                    k = first + j
                    piece = served[j * SLOTS : (j + 1) * SLOTS]
                    if k == 0:
                        ret[t, 0, c] = piece
                    else:
                        obuf[k, c] = piece
            for k in range(max(first, 1), first + GROUP):
                send = pltpu.make_async_remote_copy(
                    obuf.at[k], ret.at[t, k], ret_send.at[k], ret_recv.at[t, k],
                    device_id={"expert": source[k]}, device_id_type=MESH,
                )
                send.start()
                returns.append(send)

        moves = []
        for g in range(groups):
            first = g * GROUP
            for k in range(max(first, 1), first + GROUP):
                returns[k - 1].wait_recv()
            for c in range(CHUNKS):
                rows = ret[t, first : first + GROUP, c].reshape(GROUP * SLOTS, part)
                term = jnp.dot(mixing[t, g], rows, preferred_element_type=F32)
                total = (hid[t, c].astype(F32) if g == 0 else acc[c]) + term
                if g < groups - 1:
                    acc[c] = total
                else:
                    ybuf[c] = total.astype(BF16)
                    move = pltpu.make_async_remote_copy(
                        ybuf.at[c], hid.at[t + 1, c], y_send.at[c], y_recv.at[t, c],
                        device_id={"section": following}, device_id_type=MESH,
                    )
                    move.start()
                    moves.append(move)
        for send in sends + returns:
            send.wait_send()
        for move in moves:
            move.wait()
        return carry

    lax.fori_loop(0, ticks, tick, 0)
    stores = [
        pltpu.make_async_copy(hid.at[ticks, c], out_ref.at[:, pl.ds(c * part, part)], out_sem.at[c])
        for c in range(CHUNKS)
    ]
    for store in stores:
        store.start()
    for store in stores:
        store.wait()


def on_device(state, norm_gain, expert_in, expert_out, route_ids, route_weights):
    hidden = state[0]
    tokens, width = hidden.shape
    ticks = route_ids.shape[0]
    ff = expert_out.shape[2]
    peers = SIDE * SIDE
    part = width // CHUNKS
    vmem = pl.BlockSpec(memory_space=pltpu.VMEM)
    hbm = pl.BlockSpec(memory_space=pl.ANY)
    dma = pltpu.SemaphoreType.DMA
    result = pl.pallas_call(
        body,
        out_shape=jax.ShapeDtypeStruct((tokens, width), BF16),
        in_specs=[vmem, vmem, vmem, hbm, hbm, hbm],
        out_specs=hbm,
        scratch_shapes=[
            pltpu.VMEM((ticks + 1, CHUNKS, tokens, part), BF16),
            pltpu.VMEM((tokens, width), BF16),
            pltpu.VMEM((peers, SLOTS, width), BF16),
            pltpu.VMEM((ticks, peers, SLOTS, width), BF16),
            pltpu.VMEM((peers, CHUNKS, SLOTS, part), BF16),
            pltpu.VMEM((ticks, peers, CHUNKS, SLOTS, part), BF16),
            pltpu.VMEM((CHUNKS, tokens, part), F32),
            pltpu.VMEM((CHUNKS, tokens, part), BF16),
            pltpu.VMEM((width, 2 * ff), BF16),
            pltpu.VMEM((ff, width), BF16),
            pltpu.VMEM((GROUP * SLOTS, ff), BF16),
            pltpu.VMEM((peers, tokens), F32),
            pltpu.VMEM((peers, tokens), F32),
            pltpu.VMEM((ticks, peers, SLOTS, tokens), BF16),
            pltpu.VMEM((ticks, peers // GROUP, tokens, GROUP * SLOTS), BF16),
            dma((CHUNKS,)),
            dma((2,)),
            dma((CHUNKS,)),
            dma((peers,)),
            dma((ticks, peers)),
            dma((peers,)),
            dma((ticks, peers)),
            dma((CHUNKS,)),
            dma((ticks, CHUNKS)),
        ],
        compiler_params=pltpu.CompilerParams(
            collective_id=0, has_side_effects=True, vmem_limit_bytes=56 * 1024 * 1024
        ),
    )(
        jnp.swapaxes(route_ids[:, 0], 1, 2),
        jnp.swapaxes(route_weights[:, 0], 1, 2),
        norm_gain,
        hidden,
        expert_in[0, 0],
        expert_out[0, 0],
    )
    return result[None]


def solution(mesh):
    in_specs = (
        P("section", "expert", None),
        P("section", None),
        P("section", "expert", None, None),
        P("section", "expert", None, None),
        P(None, "section", "expert", None),
        P(None, "section", "expert", None),
    )
    out_specs = P("section", "expert", None)
    return jax.shard_map(
        on_device, mesh=mesh, in_specs=in_specs, out_specs=out_specs, check_vma=False
    )
```

```python
import functools

import jax
import jax.numpy as jnp
from jax import lax
from jax.experimental import pallas as pl
from jax.experimental.pallas import tpu as pltpu
from jax.sharding import PartitionSpec as P

MESH = pl.DeviceIdType.MESH
BF16 = jnp.bfloat16
F32 = jnp.float32

EPSILON = 1e-06
SIDE = 4
SLOTS = 32
PIECES = 4
CHUNKS = 4
ORDER = (
    (0, 0), (0, 1), (0, 3), (1, 0), (3, 0), (0, 2), (1, 1), (1, 3),
    (2, 0), (3, 1), (3, 3), (1, 2), (2, 1), (2, 3), (3, 2), (2, 2),
)


def body(
    ids_hbm, weights_hbm, gain_ref, state_ref, inner_hbm, outer_hbm, out_ref,
    ids_own, ids_prev, weights_prev, hid, carried, normed, sbuf, rbuf, obuf, ret, acc,
    inner, outer, act, rank_ref, mix_ref, pick, mixing,
    load_sem, route_sem, weight_sem, out_sem, route_send, route_recv, dispatch_send, dispatch_recv,
    ret_send, ret_recv, carry_send, carry_recv,
):
    ticks, tokens = ids_own.shape[0], ids_own.shape[1]
    width = gain_ref.shape[1]
    part = width // CHUNKS
    ff = outer.shape[0]
    peers = SIDE * SIDE
    piece = SLOTS // PIECES
    batch = peers * piece
    section = lax.axis_index("section")
    sections = lax.axis_size("section")
    me = lax.axis_index("expert")
    my_x, my_y = me // SIDE, lax.rem(me, SIDE)

    def at_offset(dx, dy):
        return lax.rem(my_x + dx + SIDE, SIDE) * SIDE + lax.rem(my_y + dy + SIDE, SIDE)

    target = [at_offset(dx, dy) for dx, dy in ORDER]
    source = [at_offset(-dx, -dy) for dx, dy in ORDER]
    following = lax.rem(section + 1, sections)
    previous = lax.rem(section + sections - 1, sections)

    barrier = pltpu.get_barrier_semaphore()
    for k in range(1, peers):
        pl.semaphore_signal(barrier, 1, device_id={"expert": target[k]}, device_id_type=MESH)
    for k in range(peers):
        for other in (following, previous):
            pl.semaphore_signal(
                barrier, 1, device_id={"section": other, "expert": target[k]}, device_id_type=MESH
            )

    route = pltpu.make_async_copy(ids_hbm, ids_own, route_sem)
    route.start()
    loads = [
        pltpu.make_async_copy(state_ref.at[:, pl.ds(c * part, part)], hid.at[0, c], load_sem.at[c])
        for c in range(CHUNKS)
    ]
    for load in loads:
        load.start()
    inner_load = pltpu.make_async_copy(inner_hbm, inner, weight_sem.at[0])
    outer_load = pltpu.make_async_copy(outer_hbm, outer, weight_sem.at[1])
    inner_load.start()
    outer_load.start()

    expert_of = lax.broadcasted_iota(jnp.int32, (peers, tokens), 0).astype(F32)
    before = lax.broadcasted_iota(jnp.int32, (tokens, tokens), 0)
    after = lax.broadcasted_iota(jnp.int32, (tokens, tokens), 1)
    earlier = jnp.where(before < after, 1.0, 0.0).astype(BF16)
    same = jnp.where(before == after, 1.0, 0.0).astype(BF16)
    slot_of = lax.broadcasted_iota(jnp.int32, (SLOTS, tokens), 0).astype(F32)

    def across(columns):
        return lax.dot_general(
            columns.astype(BF16), same, (((0,), (0,)), ((), ())), preferred_element_type=F32
        )

    def ranks(ids):
        picked = jnp.zeros((peers, tokens), F32)
        for k in range(ids.shape[0]):
            picked = jnp.where(ids[k : k + 1] == expert_of, 1.0, picked)
        rank = jnp.dot(picked.astype(BF16), earlier, preferred_element_type=F32)
        rank_ref[...] = jnp.where(picked > 0.0, rank, -1.0)

    def own_tables(t, carry):
        ranks(across(ids_own[t].astype(F32)))
        for k in range(peers):
            match = rank_ref[pl.ds(target[k], 1), :] == slot_of
            chosen = jnp.where(match, 1.0, 0.0).astype(BF16)
            for g in range(PIECES):
                pick[t, g, k] = chosen[g * piece : (g + 1) * piece]
        return carry

    def previous_tables(t, carry):
        ids, weights = across(ids_prev[t].astype(F32)), across(weights_prev[t])
        ranks(ids)
        mix = jnp.zeros((peers, tokens), F32)
        for k in range(ids.shape[0]):
            mix = jnp.where(ids[k : k + 1] == expert_of, weights[k : k + 1], mix)
        mix_ref[...] = mix
        rows = []
        for k in range(peers):
            match = rank_ref[pl.ds(target[k], 1), :] == slot_of
            rows.append(jnp.where(match, mix_ref[pl.ds(target[k], 1), :], 0.0))
        for g in range(PIECES):
            part_rows = [row[g * piece : (g + 1) * piece] for row in rows]
            mixing[t, g] = jnp.concatenate(part_rows, axis=0).T.astype(BF16)
        return carry

    route.wait()
    lax.fori_loop(0, ticks, own_tables, 0)
    for load in loads:
        load.wait()
    pl.semaphore_wait(barrier, 3 * peers - 1)
    forwards = [
        pltpu.make_async_remote_copy(
            held, landing, route_send.at[i], route_recv.at[i],
            device_id={"section": following}, device_id_type=MESH,
        )
        for i, (held, landing) in enumerate([(ids_hbm, ids_prev), (weights_hbm, weights_prev)])
    ]
    for forward in forwards:
        forward.start()

    def tick(t, carry):
        carry_on = pltpu.make_async_remote_copy(
            hid.at[t], carried.at[t], carry_send, carry_recv.at[t],
            device_id={"section": following}, device_id_type=MESH,
        )
        carry_on.start()
        squares = jnp.zeros((tokens, 1), F32)
        for c in range(CHUNKS):
            h = hid[t, c].astype(F32)
            squares = squares + jnp.sum(h * h, axis=-1, keepdims=True)
        rescale = lax.rsqrt(squares / width + EPSILON)
        for c in range(CHUNKS):
            columns = slice(c * part, (c + 1) * part)
            normed[:, columns] = (hid[t, c].astype(F32) * rescale * gain_ref[:, columns]).astype(BF16)

        sends = {}
        for g in range(PIECES):
            choose = pick[t, g].reshape(batch, tokens)
            for c in range(CHUNKS):
                columns = slice(c * part, (c + 1) * part)
                rows = jnp.dot(choose, normed[:, columns], preferred_element_type=F32).astype(BF16)
                rbuf[t, g, 0, :, columns] = rows[:piece]
                for k in range(1, peers):
                    sbuf[g, k, :, columns] = rows[k * piece : (k + 1) * piece]
            for k in range(1, peers):
                send = pltpu.make_async_remote_copy(
                    sbuf.at[g, k], rbuf.at[t, g, k], dispatch_send.at[g, k], dispatch_recv.at[t, g, k],
                    device_id={"expert": target[k]}, device_id_type=MESH,
                )
                send.start()
                sends[g, k] = send

        @pl.when(t == 0)
        def _():
            inner_load.wait()
            outer_load.wait()

        returns = {}
        for g in range(PIECES):
            for k in range(1, peers):
                sends[g, k].wait_recv()
            for n in range(ff // 256):
                gate_columns = slice(n * 256, (n + 1) * 256)
                up_columns = slice(ff + n * 256, ff + (n + 1) * 256)
                rows = rbuf[t, g].reshape(batch, width)
                gate = jnp.dot(rows, inner[:, gate_columns], preferred_element_type=F32)
                up = jnp.dot(rows, inner[:, up_columns], preferred_element_type=F32)
                act[:, gate_columns] = (gate / (1.0 + jnp.exp(-gate)) * up).astype(BF16)
            for c in range(CHUNKS):
                columns = slice(c * part, (c + 1) * part)
                served = jnp.dot(act[...], outer[:, columns], preferred_element_type=F32).astype(BF16)
                for k in range(peers):
                    obuf[g, k, :, columns] = served[k * piece : (k + 1) * piece]
            for k in range(peers):
                send = pltpu.make_async_remote_copy(
                    obuf.at[g, k], ret.at[t, g, k], ret_send.at[g, k], ret_recv.at[t, g, k],
                    device_id={"section": following, "expert": source[k]}, device_id_type=MESH,
                )
                send.start()
                returns[g, k] = send

        @pl.when(t == 0)
        def _():
            for forward in forwards:
                forward.wait()
            lax.fori_loop(0, ticks, previous_tables, 0)

        carry_on.wait_recv()
        for g in range(PIECES):
            for k in range(peers):
                returns[g, k].wait_recv()
            for c in range(CHUNKS):
                rows = ret[t, g, :, :, c * part : (c + 1) * part].reshape(batch, part)
                term = jnp.dot(mixing[t, g], rows, preferred_element_type=F32)
                total = (carried[t, c].astype(F32) if g == 0 else acc[c]) + term
                if g < PIECES - 1:
                    acc[c] = total
                else:
                    hid[t + 1, c] = total.astype(BF16)
        for send in [*sends.values(), *returns.values(), carry_on]:
            send.wait_send()
        return carry

    lax.fori_loop(0, ticks, tick, 0)
    stores = [
        pltpu.make_async_copy(hid.at[ticks, c], out_ref.at[:, pl.ds(c * part, part)], out_sem.at[c])
        for c in range(CHUNKS)
    ]
    for store in stores:
        store.start()
    for store in stores:
        store.wait()


def on_device(state, norm_gain, expert_in, expert_out, route_ids, route_weights):
    hidden = state[0]
    tokens, width = hidden.shape
    ticks, top = route_ids.shape[0], route_ids.shape[3]
    ff = expert_out.shape[2]
    peers = SIDE * SIDE
    piece = SLOTS // PIECES
    part = width // CHUNKS
    vmem = pl.BlockSpec(memory_space=pltpu.VMEM)
    hbm = pl.BlockSpec(memory_space=pl.ANY)
    dma = pltpu.SemaphoreType.DMA
    result = pl.pallas_call(
        body,
        out_shape=jax.ShapeDtypeStruct((tokens, width), BF16),
        in_specs=[hbm, hbm, vmem, hbm, hbm, hbm],
        out_specs=hbm,
        scratch_shapes=[
            pltpu.VMEM((ticks, tokens, top), jnp.int32),
            pltpu.VMEM((ticks, tokens, top), jnp.int32),
            pltpu.VMEM((ticks, tokens, top), F32),
            pltpu.VMEM((ticks + 1, CHUNKS, tokens, part), BF16),
            pltpu.VMEM((ticks, CHUNKS, tokens, part), BF16),
            pltpu.VMEM((tokens, width), BF16),
            pltpu.VMEM((PIECES, peers, piece, width), BF16),
            pltpu.VMEM((ticks, PIECES, peers, piece, width), BF16),
            pltpu.VMEM((PIECES, peers, piece, width), BF16),
            pltpu.VMEM((ticks, PIECES, peers, piece, width), BF16),
            pltpu.VMEM((CHUNKS, tokens, part), F32),
            pltpu.VMEM((width, 2 * ff), BF16),
            pltpu.VMEM((ff, width), BF16),
            pltpu.VMEM((peers * piece, ff), BF16),
            pltpu.VMEM((peers, tokens), F32),
            pltpu.VMEM((peers, tokens), F32),
            pltpu.VMEM((ticks, PIECES, peers, piece, tokens), BF16),
            pltpu.VMEM((ticks, PIECES, tokens, peers * piece), BF16),
            dma((CHUNKS,)),
            dma(()),
            dma((2,)),
            dma((CHUNKS,)),
            dma((2,)),
            dma((2,)),
            dma((PIECES, peers)),
            dma((ticks, PIECES, peers)),
            dma((PIECES, peers)),
            dma((ticks, PIECES, peers)),
            dma(()),
            dma((ticks,)),
        ],
        compiler_params=pltpu.CompilerParams(
            collective_id=0, has_side_effects=True, vmem_limit_bytes=56 * 1024 * 1024
        ),
    )(
        route_ids[:, 0],
        route_weights[:, 0],
        norm_gain,
        hidden,
        expert_in[0, 0],
        expert_out[0, 0],
    )
    return result[None]


def solution(mesh):
    in_specs = (
        P("section", "expert", None),
        P("section", None),
        P("section", "expert", None, None),
        P("section", "expert", None, None),
        P(None, "section", "expert", None),
        P(None, "section", "expert", None),
    )
    out_specs = P("section", "expert", None)
    return jax.shard_map(
        on_device, mesh=mesh, in_specs=in_specs, out_specs=out_specs, check_vma=False
    )
```

```python
import functools

import jax
import jax.numpy as jnp
from jax import lax
from jax.experimental import pallas as pl
from jax.experimental.pallas import tpu as pltpu
from jax.sharding import PartitionSpec as P

MESH = pl.DeviceIdType.MESH
BF16 = jnp.bfloat16
F32 = jnp.float32

EPSILON = 1e-06
SIDE = 4
SLOTS = 32
PIECES = 4
CHUNKS = 4
ORDER = (
    (0, 0), (0, 1), (0, 3), (1, 0), (3, 0), (0, 2), (1, 1), (1, 3),
    (2, 0), (3, 1), (3, 3), (1, 2), (2, 1), (2, 3), (3, 2), (2, 2),
)


def body(
    ids_hbm, weights_hbm, gain_ref, state_ref, inner_hbm, outer_hbm, out_ref,
    ids_own, ids_prev, weights_prev, hid, carried, normed, sbuf, rbuf, obuf, ret, acc,
    inner, outer, act, rank_ref, mix_ref, pick, mixing,
    load_sem, route_sem, weight_sem, out_sem, route_send, route_recv, dispatch_send, dispatch_recv,
    ret_send, ret_recv, carry_send, carry_recv,
):
    ticks, top, _, tokens = ids_own.shape
    width = gain_ref.shape[1]
    part = width // CHUNKS
    ff = outer.shape[0]
    peers = SIDE * SIDE
    piece = SLOTS // PIECES
    batch = peers * piece
    section = lax.axis_index("section")
    sections = lax.axis_size("section")
    me = lax.axis_index("expert")
    my_x, my_y = me // SIDE, lax.rem(me, SIDE)

    def at_offset(dx, dy):
        return lax.rem(my_x + dx + SIDE, SIDE) * SIDE + lax.rem(my_y + dy + SIDE, SIDE)

    target = [at_offset(dx, dy) for dx, dy in ORDER]
    source = [at_offset(-dx, -dy) for dx, dy in ORDER]
    following = lax.rem(section + 1, sections)
    previous = lax.rem(section + sections - 1, sections)

    barrier = pltpu.get_barrier_semaphore()
    for k in range(1, peers):
        pl.semaphore_signal(barrier, 1, device_id={"expert": target[k]}, device_id_type=MESH)
    for k in range(peers):
        for other in (following, previous):
            pl.semaphore_signal(
                barrier, 1, device_id={"section": other, "expert": target[k]}, device_id_type=MESH
            )

    route = pltpu.make_async_copy(ids_hbm, ids_own, route_sem)
    route.start()
    loads = [
        pltpu.make_async_copy(state_ref.at[:, pl.ds(c * part, part)], hid.at[0, c], load_sem.at[c])
        for c in range(CHUNKS)
    ]
    for load in loads:
        load.start()
    inner_load = pltpu.make_async_copy(inner_hbm, inner, weight_sem.at[0])
    outer_load = pltpu.make_async_copy(outer_hbm, outer, weight_sem.at[1])
    inner_load.start()
    outer_load.start()

    expert_of = lax.broadcasted_iota(jnp.int32, (peers, tokens), 0)
    before = lax.broadcasted_iota(jnp.int32, (tokens, tokens), 0)
    after = lax.broadcasted_iota(jnp.int32, (tokens, tokens), 1)
    earlier = jnp.where(before < after, 1.0, 0.0).astype(BF16)
    slot_of = lax.broadcasted_iota(jnp.int32, (SLOTS, tokens), 0).astype(F32)

    def ranks(ids):
        picked = jnp.zeros((peers, tokens), F32)
        for k in range(top):
            picked = jnp.where(ids[k] == expert_of, 1.0, picked)
        rank = jnp.dot(picked.astype(BF16), earlier, preferred_element_type=F32)
        rank_ref[...] = jnp.where(picked > 0.0, rank, -1.0)

    def own_tables(t, carry):
        ranks([ids_own[t, k] for k in range(top)])
        for k in range(peers):
            match = rank_ref[pl.ds(target[k], 1), :] == slot_of
            chosen = jnp.where(match, 1.0, 0.0).astype(BF16)
            for g in range(PIECES):
                pick[t, g, k] = chosen[g * piece : (g + 1) * piece]
        return carry

    def previous_tables(t, carry):
        ids = [ids_prev[t, k] for k in range(top)]
        ranks(ids)
        mix = jnp.zeros((peers, tokens), F32)
        for k in range(top):
            mix = jnp.where(ids[k] == expert_of, weights_prev[t, k], mix)
        mix_ref[...] = mix
        rows = []
        for k in range(peers):
            match = rank_ref[pl.ds(target[k], 1), :] == slot_of
            rows.append(jnp.where(match, mix_ref[pl.ds(target[k], 1), :], 0.0))
        for g in range(PIECES):
            part_rows = [row[g * piece : (g + 1) * piece] for row in rows]
            mixing[t, g] = jnp.concatenate(part_rows, axis=0).T.astype(BF16)
        return carry

    route.wait()
    lax.fori_loop(0, ticks, own_tables, 0)
    for load in loads:
        load.wait()
    forwards = [
        pltpu.make_async_remote_copy(
            held, landing, route_send.at[i], route_recv.at[i],
            device_id={"section": following}, device_id_type=MESH,
        )
        for i, (held, landing) in enumerate([(ids_hbm, ids_prev), (weights_hbm, weights_prev)])
    ]

    def tick(t, carry):
        squares = jnp.zeros((tokens, 1), F32)
        for c in range(CHUNKS):
            h = hid[t, c].astype(F32)
            squares = squares + jnp.sum(h * h, axis=-1, keepdims=True)
        rescale = lax.rsqrt(squares / width + EPSILON)
        for c in range(CHUNKS):
            columns = slice(c * part, (c + 1) * part)
            normed[:, columns] = (hid[t, c].astype(F32) * rescale * gain_ref[:, columns]).astype(BF16)

        carry_on = pltpu.make_async_remote_copy(
            hid.at[t], carried.at[t], carry_send, carry_recv.at[t],
            device_id={"section": following}, device_id_type=MESH,
        )
        sends = {}
        for g in range(PIECES):
            choose = pick[t, g].reshape(batch, tokens)
            for c in range(CHUNKS):
                columns = slice(c * part, (c + 1) * part)
                rows = jnp.dot(choose, normed[:, columns], preferred_element_type=F32).astype(BF16)
                rbuf[t, g, 0, :, columns] = rows[:piece]
                for k in range(1, peers):
                    sbuf[g, k, :, columns] = rows[k * piece : (k + 1) * piece]
            if g == 0:

                @pl.when(t == 0)
                def _():
                    pl.semaphore_wait(barrier, 3 * peers - 1)

            for k in (reversed(range(1, peers)) if g == PIECES - 1 else range(1, peers)):
                send = pltpu.make_async_remote_copy(
                    sbuf.at[g, k], rbuf.at[t, g, k], dispatch_send.at[g, k], dispatch_recv.at[t, g, k],
                    device_id={"expert": target[k]}, device_id_type=MESH,
                )
                send.start()
                sends[g, k] = send
            if g == 0:
                carry_on.start()

                @pl.when(t == 0)
                def _():
                    for forward in forwards:
                        forward.start()


        @pl.when(t == 0)
        def _():
            inner_load.wait()
            outer_load.wait()

        returns = {}
        for g in range(PIECES):
            for k in range(1, peers):
                sends[g, k].wait_recv()
            for n in range(ff // 256):
                gate_columns = slice(n * 256, (n + 1) * 256)
                up_columns = slice(ff + n * 256, ff + (n + 1) * 256)
                rows = rbuf[t, g].reshape(batch, width)
                gate = jnp.dot(rows, inner[:, gate_columns], preferred_element_type=F32)
                up = jnp.dot(rows, inner[:, up_columns], preferred_element_type=F32)
                act[:, gate_columns] = (gate / (1.0 + jnp.exp(-gate)) * up).astype(BF16)
            for c in range(CHUNKS):
                columns = slice(c * part, (c + 1) * part)
                served = jnp.dot(act[...], outer[:, columns], preferred_element_type=F32).astype(BF16)
                for k in range(peers):
                    obuf[g, k, :, columns] = served[k * piece : (k + 1) * piece]
            for k in (reversed(range(peers)) if g == PIECES - 1 else range(peers)):
                send = pltpu.make_async_remote_copy(
                    obuf.at[g, k], ret.at[t, g, k], ret_send.at[g, k], ret_recv.at[t, g, k],
                    device_id={"section": following, "expert": source[k]}, device_id_type=MESH,
                )
                send.start()
                returns[g, k] = send

        @pl.when(t == 0)
        def _():
            for forward in forwards:
                forward.wait()
            lax.fori_loop(0, ticks, previous_tables, 0)

        carry_on.wait_recv()
        for g in range(PIECES):
            for k in range(peers):
                returns[g, k].wait_recv()
            for c in range(CHUNKS):
                rows = ret[t, g, :, :, c * part : (c + 1) * part].reshape(batch, part)
                term = jnp.dot(mixing[t, g], rows, preferred_element_type=F32)
                total = (carried[t, c].astype(F32) if g == 0 else acc[c]) + term
                if g < PIECES - 1:
                    acc[c] = total
                else:
                    hid[t + 1, c] = total.astype(BF16)
        for send in [*sends.values(), *returns.values(), carry_on]:
            send.wait_send()
        return carry

    lax.fori_loop(0, ticks, tick, 0)
    stores = [
        pltpu.make_async_copy(hid.at[ticks, c], out_ref.at[:, pl.ds(c * part, part)], out_sem.at[c])
        for c in range(CHUNKS)
    ]
    for store in stores:
        store.start()
    for store in stores:
        store.wait()


def on_device(state, norm_gain, expert_in, expert_out, route_ids, route_weights):
    hidden = state[0]
    tokens, width = hidden.shape
    ticks, top = route_ids.shape[0], route_ids.shape[3]
    ff = expert_out.shape[2]
    peers = SIDE * SIDE
    piece = SLOTS // PIECES
    part = width // CHUNKS
    vmem = pl.BlockSpec(memory_space=pltpu.VMEM)
    hbm = pl.BlockSpec(memory_space=pl.ANY)
    dma = pltpu.SemaphoreType.DMA
    result = pl.pallas_call(
        body,
        out_shape=jax.ShapeDtypeStruct((tokens, width), BF16),
        in_specs=[hbm, hbm, vmem, hbm, hbm, hbm],
        out_specs=hbm,
        scratch_shapes=[
            pltpu.VMEM((ticks, top, 1, tokens), jnp.int32),
            pltpu.VMEM((ticks, top, 1, tokens), jnp.int32),
            pltpu.VMEM((ticks, top, 1, tokens), F32),
            pltpu.VMEM((ticks + 1, CHUNKS, tokens, part), BF16),
            pltpu.VMEM((ticks, CHUNKS, tokens, part), BF16),
            pltpu.VMEM((tokens, width), BF16),
            pltpu.VMEM((PIECES, peers, piece, width), BF16),
            pltpu.VMEM((ticks, PIECES, peers, piece, width), BF16),
            pltpu.VMEM((PIECES, peers, piece, width), BF16),
            pltpu.VMEM((ticks, PIECES, peers, piece, width), BF16),
            pltpu.VMEM((CHUNKS, tokens, part), F32),
            pltpu.VMEM((width, 2 * ff), BF16),
            pltpu.VMEM((ff, width), BF16),
            pltpu.VMEM((peers * piece, ff), BF16),
            pltpu.VMEM((peers, tokens), F32),
            pltpu.VMEM((peers, tokens), F32),
            pltpu.VMEM((ticks, PIECES, peers, piece, tokens), BF16),
            pltpu.VMEM((ticks, PIECES, tokens, peers * piece), BF16),
            dma((CHUNKS,)),
            dma(()),
            dma((2,)),
            dma((CHUNKS,)),
            dma((2,)),
            dma((2,)),
            dma((PIECES, peers)),
            dma((ticks, PIECES, peers)),
            dma((PIECES, peers)),
            dma((ticks, PIECES, peers)),
            dma(()),
            dma((ticks,)),
        ],
        compiler_params=pltpu.CompilerParams(
            collective_id=0, has_side_effects=True, vmem_limit_bytes=56 * 1024 * 1024
        ),
    )(
        jnp.transpose(route_ids, (0, 3, 1, 2)),
        jnp.transpose(route_weights, (0, 3, 1, 2)),
        norm_gain,
        hidden,
        expert_in[0, 0],
        expert_out[0, 0],
    )
    return result[None]


def solution(mesh):
    in_specs = (
        P("section", "expert", None),
        P("section", None),
        P("section", "expert", None, None),
        P("section", "expert", None, None),
        P(None, "section", "expert", None),
        P(None, "section", "expert", None),
    )
    out_specs = P("section", "expert", None)
    return jax.shard_map(
        on_device, mesh=mesh, in_specs=in_specs, out_specs=out_specs, check_vma=False
    )
```

```python
import functools

import jax
import jax.numpy as jnp
from jax import lax
from jax.experimental import pallas as pl
from jax.experimental.pallas import tpu as pltpu
from jax.sharding import PartitionSpec as P

MESH = pl.DeviceIdType.MESH
BF16 = jnp.bfloat16
F32 = jnp.float32

EPSILON = 1e-06
SIDE = 4
SLOTS = 32
HALVES = 2
CHUNKS = 4
RETURNS = 4
ORDER = (
    (0, 0), (0, 1), (0, 3), (1, 0), (3, 0), (0, 2), (1, 1), (1, 3),
    (2, 0), (3, 1), (3, 3), (1, 2), (2, 1), (2, 3), (3, 2), (2, 2),
)
NEAR = ((0, 0), (0, 1), (0, 3), (1, 0), (0, 2), (1, 1), (1, 3), (1, 2))


def body(
    ids_hbm, weights_hbm, gain_ref, state_ref, inner_hbm, outer_hbm, out_ref,
    ids_own, ids_prev, weights_prev, ids_pair, hid, carried, normed, dense, sbuf, rbuf, obuf, ret, acc,
    inner, outer, act, rank_ref, mix_ref, pick, mixing,
    load_sem, route_sem, weight_sem, out_sem, route_send, route_recv, pair_send, pair_recv,
    dense_send, dense_recv, dispatch_send, dispatch_recv, ret_send, ret_recv, carry_send, carry_recv,
):
    ticks, top, _, tokens = ids_own.shape
    width = gain_ref.shape[1]
    part = width // CHUNKS
    ret_part = width // RETURNS
    ff = outer.shape[0]
    peers = SIDE * SIDE
    half = SLOTS // HALVES
    batch = peers * half
    section = lax.axis_index("section")
    sections = lax.axis_size("section")
    me = lax.axis_index("expert")
    my_x, my_y = me // SIDE, lax.rem(me, SIDE)

    def wrap(value):
        return lax.rem(value + 2 * SIDE, SIDE)

    def at_offset(dx, dy):
        return wrap(my_x + dx) * SIDE + wrap(my_y + dy)

    target = [at_offset(k // SIDE, k % SIDE) for k in range(peers)]
    source = [at_offset(-(k // SIDE), -(k % SIDE)) for k in range(peers)]
    order = [dx * SIDE + dy for dx, dy in ORDER]
    following = lax.rem(section + 1, sections)
    previous = lax.rem(section + sections - 1, sections)

    step_x, step_y = 1 - 2 * lax.rem(my_x, 2), 1 - 2 * lax.rem(my_y, 2)
    steps = [step_x, -step_x, step_y, -step_y]
    partner, near_target, near_index = [], [], []
    for c, step in enumerate(steps):
        along = c < CHUNKS // 2

        def offset(lengthwise, across, along=along):
            return (lengthwise, across) if along else (across, lengthwise)

        partner.append(at_offset(*offset(step, 0)))
        near_target.append([at_offset(*offset(-step * away, across)) for away, across in NEAR])
        indices = []
        for owner in range(2):
            pairs = [offset(wrap(-step * (away + owner)), across) for away, across in NEAR]
            indices.append([dx * SIDE + dy for dx, dy in pairs])
        near_index.append(indices)

    barrier = pltpu.get_barrier_semaphore()
    for k in range(1, peers):
        pl.semaphore_signal(barrier, 1, device_id={"expert": target[k]}, device_id_type=MESH)
    for k in range(peers):
        for other in (following, previous):
            pl.semaphore_signal(
                barrier, 1, device_id={"section": other, "expert": target[k]}, device_id_type=MESH
            )

    route = pltpu.make_async_copy(ids_hbm, ids_own, route_sem)
    route.start()
    loads = [
        pltpu.make_async_copy(state_ref.at[:, pl.ds(c * part, part)], hid.at[0, c], load_sem.at[c])
        for c in range(CHUNKS)
    ]
    for load in loads:
        load.start()
    inner_load = pltpu.make_async_copy(inner_hbm, inner, weight_sem.at[0])
    outer_load = pltpu.make_async_copy(outer_hbm, outer, weight_sem.at[1])
    inner_load.start()
    outer_load.start()

    expert_of = lax.broadcasted_iota(jnp.int32, (peers, tokens), 0)
    before = lax.broadcasted_iota(jnp.int32, (tokens, tokens), 0)
    after = lax.broadcasted_iota(jnp.int32, (tokens, tokens), 1)
    earlier = jnp.where(before < after, 1.0, 0.0).astype(BF16)
    slot_of = lax.broadcasted_iota(jnp.int32, (SLOTS, tokens), 0).astype(F32)

    def ranks(ids):
        picked = jnp.zeros((peers, tokens), F32)
        for k in range(top):
            picked = jnp.where(ids[k] == expert_of, 1.0, picked)
        rank = jnp.dot(picked.astype(BF16), earlier, preferred_element_type=F32)
        rank_ref[...] = jnp.where(picked > 0.0, rank, -1.0)

    def choose(t, owner, c):
        for j in range(len(NEAR)):
            match = rank_ref[pl.ds(near_target[c][j], 1), :] == slot_of
            chosen = jnp.where(match, 1.0, 0.0).astype(BF16)
            for h in range(HALVES):
                pick[t, owner, c, h, j] = chosen[h * half : (h + 1) * half]

    def own_tables(t, carry):
        ranks([ids_own[t, k] for k in range(top)])
        for c in range(CHUNKS):
            choose(t, 0, c)
        return carry

    def pair_tables(t, carry):
        for c in range(CHUNKS):
            ranks([ids_pair[c, t, k] for k in range(top)])
            choose(t, 1, c)
        return carry

    def previous_tables(t, carry):
        ids = [ids_prev[t, k] for k in range(top)]
        ranks(ids)
        mix = jnp.zeros((peers, tokens), F32)
        for k in range(top):
            mix = jnp.where(ids[k] == expert_of, weights_prev[t, k], mix)
        mix_ref[...] = mix
        rows = []
        for k in range(peers):
            match = rank_ref[pl.ds(target[k], 1), :] == slot_of
            rows.append(jnp.where(match, mix_ref[pl.ds(target[k], 1), :], 0.0))
        for h in range(HALVES):
            half_rows = [row[h * half : (h + 1) * half] for row in rows]
            mixing[t, h] = jnp.concatenate(half_rows, axis=0).T.astype(BF16)
        return carry

    route.wait()
    own_tables(0, 0)
    for load in loads:
        load.wait()
    forwards = [
        pltpu.make_async_remote_copy(
            held, landing, route_send.at[i], route_recv.at[i],
            device_id={"section": following}, device_id_type=MESH,
        )
        for i, (held, landing) in enumerate([(ids_hbm, ids_prev), (weights_hbm, weights_prev)])
    ]
    pair_routes = [
        pltpu.make_async_remote_copy(
            ids_hbm, ids_pair.at[c], pair_send.at[c], pair_recv.at[c],
            device_id={"expert": partner[c]}, device_id_type=MESH,
        )
        for c in range(CHUNKS)
    ]

    def tick(t, carry):
        squares = jnp.zeros((tokens, 1), F32)
        for c in range(CHUNKS):
            h = hid[t, c].astype(F32)
            squares = squares + jnp.sum(h * h, axis=-1, keepdims=True)
        rescale = lax.rsqrt(squares / width + EPSILON)
        for c in range(CHUNKS):
            columns = slice(c * part, (c + 1) * part)
            normed[c] = (hid[t, c].astype(F32) * rescale * gain_ref[:, columns]).astype(BF16)

        @pl.when(t == 0)
        def _():
            pl.semaphore_wait(barrier, 3 * peers - 1)
            for pair_route in pair_routes:
                pair_route.start()

        shares = [
            pltpu.make_async_remote_copy(
                normed.at[c], dense.at[t, c], dense_send.at[c], dense_recv.at[t, c],
                device_id={"expert": partner[c]}, device_id_type=MESH,
            )
            for c in range(CHUNKS)
        ]
        for share in shares:
            share.start()
        carry_on = pltpu.make_async_remote_copy(
            hid.at[t], carried.at[t], carry_send, carry_recv.at[t],
            device_id={"section": following}, device_id_type=MESH,
        )

        def serve(owner, h, reverse=False):
            for c in range(CHUNKS):
                chosen = pick[t, owner, c, h].reshape(len(NEAR) * half, tokens)
                tokens_part = normed[c] if owner == 0 else dense[t, c]
                rows = jnp.dot(chosen, tokens_part, preferred_element_type=F32).astype(BF16)
                columns = slice(c * part, (c + 1) * part)
                rbuf[t, h, near_index[c][owner][0], :, columns] = rows[:half]
                for j in range(1, len(NEAR)):
                    sbuf[h, owner, c, j] = rows[j * half : (j + 1) * half]
            numbers = list(range(1, len(NEAR)))
            for j in reversed(numbers) if reverse else numbers:
                for c in range(CHUNKS):
                    pltpu.make_async_remote_copy(
                        sbuf.at[h, owner, c, j],
                        rbuf.at[t, h, near_index[c][owner][j], :, pl.ds(c * part, part)],
                        dispatch_send.at[h], dispatch_recv.at[t, h],
                        device_id={"expert": near_target[c][j]}, device_id_type=MESH,
                    ).start()

        serve(0, 0)
        carry_on.start()

        @pl.when(t == 0)
        def _():
            for forward in forwards:
                forward.start()
            for pair_route in pair_routes:
                pair_route.wait()
            pair_tables(0, 0)

        for share in shares:
            share.wait_recv()
        serve(1, 0)
        @pl.when(t == 0)
        def _():
            lax.fori_loop(1, ticks, own_tables, 0)
            lax.fori_loop(1, ticks, pair_tables, 0)

        serve(0, 1)
        serve(1, 1)

        @pl.when(t == 0)
        def _():
            inner_load.wait()
            outer_load.wait()

        arrivals = []
        returns = []
        remote = CHUNKS * 2 * (len(NEAR) - 1) * half * part // (half * width)
        for h in range(HALVES):
            landed = rbuf.at[t, h, pl.ds(0, remote)]
            arrival = pltpu.make_async_remote_copy(
                landed, landed, dispatch_send.at[h], dispatch_recv.at[t, h],
                device_id={"expert": partner[0]}, device_id_type=MESH,
            )
            arrival.wait_recv()
            arrivals.append(arrival)
            for n in range(ff // 256):
                gate_columns = slice(n * 256, (n + 1) * 256)
                up_columns = slice(ff + n * 256, ff + (n + 1) * 256)
                rows = rbuf[t, h].reshape(batch, width)
                gate = jnp.dot(rows, inner[:, gate_columns], preferred_element_type=F32)
                up = jnp.dot(rows, inner[:, up_columns], preferred_element_type=F32)
                act[:, gate_columns] = (gate / (1.0 + jnp.exp(-gate)) * up).astype(BF16)
            for r in range(RETURNS):
                for n in range(ret_part // part):
                    columns = slice(r * ret_part + n * part, r * ret_part + (n + 1) * part)
                    served = jnp.dot(act[...], outer[:, columns], preferred_element_type=F32).astype(BF16)
                    for k in range(peers):
                        obuf[h, r, k, :, n * part : (n + 1) * part] = served[k * half : (k + 1) * half]
                last = h == HALVES - 1 and r == RETURNS - 1
                for k in order:
                    pltpu.make_async_remote_copy(
                        obuf.at[h, r, k], ret.at[t, h, r, k], ret_send.at[h, r], ret_recv.at[t, h, r],
                        device_id={"section": following, "expert": source[k]}, device_id_type=MESH,
                    ).start()
                returns.append(
                    pltpu.make_async_remote_copy(
                        obuf.at[h, r], ret.at[t, h, r], ret_send.at[h, r], ret_recv.at[t, h, r],
                        device_id={"section": following, "expert": me}, device_id_type=MESH,
                    )
                )

        @pl.when(t == 0)
        def _():
            for forward in forwards:
                forward.wait()
            lax.fori_loop(0, ticks, previous_tables, 0)

        carry_on.wait_recv()
        for h in range(HALVES):
            for r in range(RETURNS):
                returns[h * RETURNS + r].wait_recv()
                for n in range(ret_part // part):
                    c = r * (ret_part // part) + n
                    rows = ret[t, h, r, :, :, n * part : (n + 1) * part].reshape(batch, part)
                    term = jnp.dot(mixing[t, h], rows, preferred_element_type=F32)
                    total = (carried[t, c].astype(F32) if h == 0 else acc[c]) + term
                    if h < HALVES - 1:
                        acc[c] = total
                    else:
                        hid[t + 1, c] = total.astype(BF16)
        for send in [*shares, *arrivals, *returns, carry_on]:
            send.wait_send()
        return carry

    lax.fori_loop(0, ticks, tick, 0)
    stores = [
        pltpu.make_async_copy(hid.at[ticks, c], out_ref.at[:, pl.ds(c * part, part)], out_sem.at[c])
        for c in range(CHUNKS)
    ]
    for store in stores:
        store.start()
    for store in stores:
        store.wait()


def on_device(state, norm_gain, expert_in, expert_out, route_ids, route_weights):
    hidden = state[0]
    tokens, width = hidden.shape
    ticks, top = route_ids.shape[0], route_ids.shape[3]
    ff = expert_out.shape[2]
    peers = SIDE * SIDE
    half = SLOTS // HALVES
    part = width // CHUNKS
    ret_part = width // RETURNS
    near = len(NEAR)
    vmem = pl.BlockSpec(memory_space=pltpu.VMEM)
    hbm = pl.BlockSpec(memory_space=pl.ANY)
    dma = pltpu.SemaphoreType.DMA
    result = pl.pallas_call(
        body,
        out_shape=jax.ShapeDtypeStruct((tokens, width), BF16),
        in_specs=[hbm, hbm, vmem, hbm, hbm, hbm],
        out_specs=hbm,
        scratch_shapes=[
            pltpu.VMEM((ticks, top, 1, tokens), jnp.int32),
            pltpu.VMEM((ticks, top, 1, tokens), jnp.int32),
            pltpu.VMEM((ticks, top, 1, tokens), F32),
            pltpu.VMEM((CHUNKS, ticks, top, 1, tokens), jnp.int32),
            pltpu.VMEM((ticks + 1, CHUNKS, tokens, part), BF16),
            pltpu.VMEM((ticks, CHUNKS, tokens, part), BF16),
            pltpu.VMEM((CHUNKS, tokens, part), BF16),
            pltpu.VMEM((ticks, CHUNKS, tokens, part), BF16),
            pltpu.VMEM((HALVES, 2, CHUNKS, near, half, part), BF16),
            pltpu.VMEM((ticks, HALVES, peers, half, width), BF16),
            pltpu.VMEM((HALVES, RETURNS, peers, half, ret_part), BF16),
            pltpu.VMEM((ticks, HALVES, RETURNS, peers, half, ret_part), BF16),
            pltpu.VMEM((CHUNKS, tokens, part), F32),
            pltpu.VMEM((width, 2 * ff), BF16),
            pltpu.VMEM((ff, width), BF16),
            pltpu.VMEM((peers * half, ff), BF16),
            pltpu.VMEM((peers, tokens), F32),
            pltpu.VMEM((peers, tokens), F32),
            pltpu.VMEM((ticks, 2, CHUNKS, HALVES, near, half, tokens), BF16),
            pltpu.VMEM((ticks, HALVES, tokens, peers * half), BF16),
            dma((CHUNKS,)),
            dma(()),
            dma((2,)),
            dma((CHUNKS,)),
            dma((2,)),
            dma((2,)),
            dma((CHUNKS,)),
            dma((CHUNKS,)),
            dma((CHUNKS,)),
            dma((ticks, CHUNKS)),
            dma((HALVES,)),
            dma((ticks, HALVES)),
            dma((HALVES, RETURNS)),
            dma((ticks, HALVES, RETURNS)),
            dma(()),
            dma((ticks,)),
        ],
        compiler_params=pltpu.CompilerParams(
            collective_id=0, has_side_effects=True, vmem_limit_bytes=56 * 1024 * 1024
        ),
    )(
        jnp.transpose(route_ids, (0, 3, 1, 2)),
        jnp.transpose(route_weights, (0, 3, 1, 2)),
        norm_gain,
        hidden,
        expert_in[0, 0],
        expert_out[0, 0],
    )
    return result[None]


def solution(mesh):
    in_specs = (
        P("section", "expert", None),
        P("section", None),
        P("section", "expert", None, None),
        P("section", "expert", None, None),
        P(None, "section", "expert", None),
        P(None, "section", "expert", None),
    )
    out_specs = P("section", "expert", None)
    return jax.shard_map(
        on_device, mesh=mesh, in_specs=in_specs, out_specs=out_specs, check_vma=False
    )
```

```python
import functools

import jax
import jax.numpy as jnp
from jax import lax
from jax.experimental import pallas as pl
from jax.experimental.pallas import tpu as pltpu
from jax.sharding import PartitionSpec as P

MESH = pl.DeviceIdType.MESH
BF16 = jnp.bfloat16
F32 = jnp.float32

EPSILON = 1e-06
SIDE = 4
SLOTS = 32
HALVES = 2
CHUNKS = 4
RETURNS = 4
ORDER = (
    (0, 0), (0, 1), (0, 3), (1, 0), (3, 0), (0, 2), (1, 1), (1, 3),
    (2, 0), (3, 1), (3, 3), (1, 2), (2, 1), (2, 3), (3, 2), (2, 2),
)
NEAR = ((0, 0), (0, 1), (0, 3), (1, 0), (0, 2), (1, 1), (1, 3), (1, 2))


def body(
    ids_hbm, weights_hbm, gain_ref, state_ref, inner_hbm, outer_hbm, out_ref,
    ids_own, ids_prev, weights_prev, ids_pair, hid, carried, normed, dense, sbuf, rbuf, obuf, ret, acc,
    inner, outer, act, rank_ref, mix_ref, pick, mixing,
    load_sem, route_sem, weight_sem, out_sem, route_send, route_recv, pair_send, pair_recv,
    dense_send, dense_recv, dispatch_send, dispatch_recv, ret_send, ret_recv, carry_send, carry_recv,
):
    ticks, top, _, tokens = ids_own.shape
    width = gain_ref.shape[1]
    part = width // CHUNKS
    ret_part = width // RETURNS
    ff = outer.shape[0]
    peers = SIDE * SIDE
    half = SLOTS // HALVES
    batch = peers * half
    section = lax.axis_index("section")
    sections = lax.axis_size("section")
    me = lax.axis_index("expert")
    my_x, my_y = me // SIDE, lax.rem(me, SIDE)

    def wrap(value):
        return lax.rem(value + 2 * SIDE, SIDE)

    def at_offset(dx, dy):
        return wrap(my_x + dx) * SIDE + wrap(my_y + dy)

    target = [at_offset(k // SIDE, k % SIDE) for k in range(peers)]
    source = [at_offset(-(k // SIDE), -(k % SIDE)) for k in range(peers)]
    order = [dx * SIDE + dy for dx, dy in ORDER]
    following = lax.rem(section + 1, sections)
    previous = lax.rem(section + sections - 1, sections)

    step_x, step_y = 1 - 2 * lax.rem(my_x, 2), 1 - 2 * lax.rem(my_y, 2)
    steps = [step_x, -step_x, step_y, -step_y]
    partner, near_target, near_index = [], [], []
    for c, step in enumerate(steps):
        along = c < CHUNKS // 2

        def offset(lengthwise, across, along=along):
            return (lengthwise, across) if along else (across, lengthwise)

        partner.append(at_offset(*offset(step, 0)))
        near_target.append([at_offset(*offset(-step * away, across)) for away, across in NEAR])
        indices = []
        for owner in range(2):
            pairs = [offset(wrap(-step * (away + owner)), across) for away, across in NEAR]
            indices.append([dx * SIDE + dy for dx, dy in pairs])
        near_index.append(indices)

    barrier = pltpu.get_barrier_semaphore()
    for k in range(1, peers):
        pl.semaphore_signal(barrier, 1, device_id={"expert": target[k]}, device_id_type=MESH)
    for k in range(peers):
        for other in (following, previous):
            pl.semaphore_signal(
                barrier, 1, device_id={"section": other, "expert": target[k]}, device_id_type=MESH
            )

    route = pltpu.make_async_copy(ids_hbm, ids_own, route_sem)
    route.start()
    loads = [
        pltpu.make_async_copy(state_ref.at[:, pl.ds(c * part, part)], hid.at[0, c], load_sem.at[c])
        for c in range(CHUNKS)
    ]
    for load in loads:
        load.start()
    inner_load = pltpu.make_async_copy(inner_hbm, inner, weight_sem.at[0])
    outer_load = pltpu.make_async_copy(outer_hbm, outer, weight_sem.at[1])
    inner_load.start()
    outer_load.start()

    expert_of = lax.broadcasted_iota(jnp.int32, (peers, tokens), 0)
    before = lax.broadcasted_iota(jnp.int32, (tokens, tokens), 0)
    after = lax.broadcasted_iota(jnp.int32, (tokens, tokens), 1)
    earlier = jnp.where(before < after, 1.0, 0.0).astype(BF16)
    slot_of = lax.broadcasted_iota(jnp.int32, (SLOTS, tokens), 0).astype(F32)

    def ranks(ids):
        picked = jnp.zeros((peers, tokens), F32)
        for k in range(top):
            picked = jnp.where(ids[k] == expert_of, 1.0, picked)
        rank = jnp.dot(picked.astype(BF16), earlier, preferred_element_type=F32)
        rank_ref[...] = jnp.where(picked > 0.0, rank, -1.0)

    def choose(t, owner, c):
        for j in range(len(NEAR)):
            match = rank_ref[pl.ds(near_target[c][j], 1), :] == slot_of
            chosen = jnp.where(match, 1.0, 0.0).astype(BF16)
            for h in range(HALVES):
                pick[t, owner, c, h, j] = chosen[h * half : (h + 1) * half]

    def own_tables(t, carry):
        ranks([ids_own[t, k] for k in range(top)])
        for c in range(CHUNKS):
            choose(t, 0, c)
        return carry

    def pair_tables(t, carry):
        for c in range(CHUNKS):
            ranks([ids_pair[c, t, k] for k in range(top)])
            choose(t, 1, c)
        return carry

    def previous_tables(t, carry):
        ids = [ids_prev[t, k] for k in range(top)]
        ranks(ids)
        mix = jnp.zeros((peers, tokens), F32)
        for k in range(top):
            mix = jnp.where(ids[k] == expert_of, weights_prev[t, k], mix)
        mix_ref[...] = mix
        rows = []
        for k in range(peers):
            match = rank_ref[pl.ds(target[k], 1), :] == slot_of
            rows.append(jnp.where(match, mix_ref[pl.ds(target[k], 1), :], 0.0))
        for h in range(HALVES):
            half_rows = [row[h * half : (h + 1) * half] for row in rows]
            mixing[t, h] = jnp.concatenate(half_rows, axis=0).T.astype(BF16)
        return carry

    route.wait()
    own_tables(0, 0)
    for load in loads:
        load.wait()
    forwards = [
        pltpu.make_async_remote_copy(
            held, landing, route_send.at[i], route_recv.at[i],
            device_id={"section": following}, device_id_type=MESH,
        )
        for i, (held, landing) in enumerate([(ids_hbm, ids_prev), (weights_hbm, weights_prev)])
    ]
    pair_routes = [
        pltpu.make_async_remote_copy(
            ids_hbm, ids_pair.at[c], pair_send.at[c], pair_recv.at[c],
            device_id={"expert": partner[c]}, device_id_type=MESH,
        )
        for c in range(CHUNKS)
    ]

    stores = [
        pltpu.make_async_copy(hid.at[ticks, c], out_ref.at[:, pl.ds(c * part, part)], out_sem.at[c])
        for c in range(CHUNKS)
    ]

    def tick(t, carry):
        squares = jnp.zeros((tokens, 1), F32)
        for c in range(CHUNKS):
            h = hid[t, c].astype(F32)
            squares = squares + jnp.sum(h * h, axis=-1, keepdims=True)
        rescale = lax.rsqrt(squares / width + EPSILON)
        for c in range(CHUNKS):
            columns = slice(c * part, (c + 1) * part)
            normed[c] = (hid[t, c].astype(F32) * rescale * gain_ref[:, columns]).astype(BF16)

        @pl.when(t == 0)
        def _():
            pl.semaphore_wait(barrier, 3 * peers - 1)
            for pair_route in pair_routes:
                pair_route.start()

        shares = [
            pltpu.make_async_remote_copy(
                normed.at[c], dense.at[t, c], dense_send.at[c], dense_recv.at[t, c],
                device_id={"expert": partner[c]}, device_id_type=MESH,
            )
            for c in range(CHUNKS)
        ]
        for share in shares:
            share.start()
        carry_on = pltpu.make_async_remote_copy(
            hid.at[t], carried.at[t], carry_send, carry_recv.at[t],
            device_id={"section": following}, device_id_type=MESH,
        )

        def serve(owner, h, reverse=False):
            for c in range(CHUNKS):
                chosen = pick[t, owner, c, h].reshape(len(NEAR) * half, tokens)
                tokens_part = normed[c] if owner == 0 else dense[t, c]
                rows = jnp.dot(chosen, tokens_part, preferred_element_type=F32).astype(BF16)
                columns = slice(c * part, (c + 1) * part)
                rbuf[t, h, near_index[c][owner][0], :, columns] = rows[:half]
                for j in range(1, len(NEAR)):
                    sbuf[h, owner, c, j] = rows[j * half : (j + 1) * half]
            numbers = list(range(1, len(NEAR)))
            for j in reversed(numbers) if reverse else numbers:
                for c in range(CHUNKS):
                    pltpu.make_async_remote_copy(
                        sbuf.at[h, owner, c, j],
                        rbuf.at[t, h, near_index[c][owner][j], :, pl.ds(c * part, part)],
                        dispatch_send.at[h], dispatch_recv.at[t, h],
                        device_id={"expert": near_target[c][j]}, device_id_type=MESH,
                    ).start()

        serve(0, 0)
        carry_on.start()

        @pl.when(t == 0)
        def _():
            for forward in forwards:
                forward.start()
            for pair_route in pair_routes:
                pair_route.wait()
            pair_tables(0, 0)

        for share in shares:
            share.wait_recv()
        serve(1, 0)
        @pl.when(t == 0)
        def _():
            lax.fori_loop(1, ticks, own_tables, 0)
            lax.fori_loop(1, ticks, pair_tables, 0)

        serve(0, 1)
        serve(1, 1)

        @pl.when(t == 0)
        def _():
            inner_load.wait()
            outer_load.wait()

        arrivals = []
        returns = []
        remote = CHUNKS * 2 * (len(NEAR) - 1) * half * part // (half * width)
        for h in range(HALVES):
            landed = rbuf.at[t, h, pl.ds(0, remote)]
            arrival = pltpu.make_async_remote_copy(
                landed, landed, dispatch_send.at[h], dispatch_recv.at[t, h],
                device_id={"expert": partner[0]}, device_id_type=MESH,
            )
            arrival.wait_recv()
            arrivals.append(arrival)
            for n in range(ff // 256):
                gate_columns = slice(n * 256, (n + 1) * 256)
                up_columns = slice(ff + n * 256, ff + (n + 1) * 256)
                rows = rbuf[t, h].reshape(batch, width)
                gate = jnp.dot(rows, inner[:, gate_columns], preferred_element_type=F32)
                up = jnp.dot(rows, inner[:, up_columns], preferred_element_type=F32)
                act[:, gate_columns] = (gate / (1.0 + jnp.exp(-gate)) * up).astype(BF16)
            for r in range(RETURNS):
                for n in range(ret_part // part):
                    columns = slice(r * ret_part + n * part, r * ret_part + (n + 1) * part)
                    served = jnp.dot(act[...], outer[:, columns], preferred_element_type=F32).astype(BF16)
                    for k in range(peers):
                        obuf[h, r, k, :, n * part : (n + 1) * part] = served[k * half : (k + 1) * half]
                last = h == HALVES - 1 and r == RETURNS - 1
                for k in order:
                    pltpu.make_async_remote_copy(
                        obuf.at[h, r, k], ret.at[t, h, r, k], ret_send.at[h, r], ret_recv.at[t, h, r],
                        device_id={"section": following, "expert": source[k]}, device_id_type=MESH,
                    ).start()
                returns.append(
                    pltpu.make_async_remote_copy(
                        obuf.at[h, r], ret.at[t, h, r], ret_send.at[h, r], ret_recv.at[t, h, r],
                        device_id={"section": following, "expert": me}, device_id_type=MESH,
                    )
                )

        @pl.when(t == 0)
        def _():
            for forward in forwards:
                forward.wait()
            lax.fori_loop(0, ticks, previous_tables, 0)

        carry_on.wait_recv()
        for h in range(HALVES):
            for r in range(RETURNS):
                returns[h * RETURNS + r].wait_recv()
                for n in range(ret_part // part):
                    c = r * (ret_part // part) + n
                    rows = ret[t, h, r, :, :, n * part : (n + 1) * part].reshape(batch, part)
                    term = jnp.dot(mixing[t, h], rows, preferred_element_type=F32)
                    total = (carried[t, c].astype(F32) if h == 0 else acc[c]) + term
                    if h < HALVES - 1:
                        acc[c] = total
                    else:
                        hid[t + 1, c] = total.astype(BF16)
                        if c > 0:

                            @pl.when(t == ticks - 1)
                            def _(c=c):
                                stores[c - 1].start()

        for send in [*shares, *arrivals, *returns, carry_on]:
            send.wait_send()
        return carry

    lax.fori_loop(0, ticks, tick, 0)
    stores[-1].start()
    for store in stores:
        store.wait()


def on_device(state, norm_gain, expert_in, expert_out, route_ids, route_weights):
    hidden = state[0]
    tokens, width = hidden.shape
    ticks, top = route_ids.shape[0], route_ids.shape[3]
    ff = expert_out.shape[2]
    peers = SIDE * SIDE
    half = SLOTS // HALVES
    part = width // CHUNKS
    ret_part = width // RETURNS
    near = len(NEAR)
    vmem = pl.BlockSpec(memory_space=pltpu.VMEM)
    hbm = pl.BlockSpec(memory_space=pl.ANY)
    dma = pltpu.SemaphoreType.DMA
    result = pl.pallas_call(
        body,
        out_shape=jax.ShapeDtypeStruct((tokens, width), BF16),
        in_specs=[hbm, hbm, vmem, hbm, hbm, hbm],
        out_specs=hbm,
        scratch_shapes=[
            pltpu.VMEM((ticks, top, 1, tokens), jnp.int32),
            pltpu.VMEM((ticks, top, 1, tokens), jnp.int32),
            pltpu.VMEM((ticks, top, 1, tokens), F32),
            pltpu.VMEM((CHUNKS, ticks, top, 1, tokens), jnp.int32),
            pltpu.VMEM((ticks + 1, CHUNKS, tokens, part), BF16),
            pltpu.VMEM((ticks, CHUNKS, tokens, part), BF16),
            pltpu.VMEM((CHUNKS, tokens, part), BF16),
            pltpu.VMEM((ticks, CHUNKS, tokens, part), BF16),
            pltpu.VMEM((HALVES, 2, CHUNKS, near, half, part), BF16),
            pltpu.VMEM((ticks, HALVES, peers, half, width), BF16),
            pltpu.VMEM((HALVES, RETURNS, peers, half, ret_part), BF16),
            pltpu.VMEM((ticks, HALVES, RETURNS, peers, half, ret_part), BF16),
            pltpu.VMEM((CHUNKS, tokens, part), F32),
            pltpu.VMEM((width, 2 * ff), BF16),
            pltpu.VMEM((ff, width), BF16),
            pltpu.VMEM((peers * half, ff), BF16),
            pltpu.VMEM((peers, tokens), F32),
            pltpu.VMEM((peers, tokens), F32),
            pltpu.VMEM((ticks, 2, CHUNKS, HALVES, near, half, tokens), BF16),
            pltpu.VMEM((ticks, HALVES, tokens, peers * half), BF16),
            dma((CHUNKS,)),
            dma(()),
            dma((2,)),
            dma((CHUNKS,)),
            dma((2,)),
            dma((2,)),
            dma((CHUNKS,)),
            dma((CHUNKS,)),
            dma((CHUNKS,)),
            dma((ticks, CHUNKS)),
            dma((HALVES,)),
            dma((ticks, HALVES)),
            dma((HALVES, RETURNS)),
            dma((ticks, HALVES, RETURNS)),
            dma(()),
            dma((ticks,)),
        ],
        compiler_params=pltpu.CompilerParams(
            collective_id=0, has_side_effects=True, vmem_limit_bytes=56 * 1024 * 1024
        ),
    )(
        jnp.transpose(route_ids, (0, 3, 1, 2)),
        jnp.transpose(route_weights, (0, 3, 1, 2)),
        norm_gain,
        hidden,
        expert_in[0, 0],
        expert_out[0, 0],
    )
    return result[None]


def solution(mesh):
    in_specs = (
        P("section", "expert", None),
        P("section", None),
        P("section", "expert", None, None),
        P("section", "expert", None, None),
        P(None, "section", "expert", None),
        P(None, "section", "expert", None),
    )
    out_specs = P("section", "expert", None)
    return jax.shard_map(
        on_device, mesh=mesh, in_specs=in_specs, out_specs=out_specs, check_vma=False
    )
```
